8 devices in a mesh: local: 2 (over z, y), data: 4 (over x, core).
Axes of the slice: x: 2, y: 2, z: 1, core: 2. Of those that a mesh axis runs over, the one named last changes fastest.
Arguments:
- tokens: bfloat16 [16384, 1536], P(('local', 'data'))
- grad_out: bfloat16 [16384, 1536], P(('local', 'data'))
- w_up: bfloat16 [2, 1536, 8960], P(None, ('local', 'data'))
- w_down: bfloat16 [2, 8960, 1536], P(None, ('local', 'data'))
Outputs:
- output 1: bfloat16 [16384, 1536], P(('local', 'data'))
- output 2: bfloat16 [16384, 1536], P(('local', 'data'))
- output 3: float32 [2, 1536, 8960], P(None, ('local', 'data'))
- output 4: float32 [2, 8960, 1536], P(None, ('local', 'data'))
All inputs are finite; a program needn't handle non-finite values.
Results may differ from the reference program's by a relative error of at most 0.0119238.
Values are sent between devices in bfloat16 or wider.
A program may use at most 1 GiB of HBM per device.

```python
import jax
import jax.numpy as jnp
from jax import lax

HIDDEN = 1536
FFN_DIM = 8960
NUM_LAYERS = 2
TOTAL_TOKENS = 16384
NORM_EPS = 1e-6
BLOCK_ROWS = min(TOTAL_TOKENS, 2048)


def setup_inputs(seed: int = 0) -> dict:
    keys = jax.random.split(jax.random.key(seed), 4)
    tokens = jax.random.normal(keys[0], (TOTAL_TOKENS, HIDDEN), jnp.float32).astype(jnp.bfloat16)
    grad_out = jax.random.normal(keys[1], (TOTAL_TOKENS, HIDDEN), jnp.float32).astype(jnp.bfloat16)
    w_up = (jax.random.normal(keys[2], (NUM_LAYERS, HIDDEN, FFN_DIM), jnp.float32) * HIDDEN ** -0.5).astype(jnp.bfloat16)
    w_down = (jax.random.normal(keys[3], (NUM_LAYERS, FFN_DIM, HIDDEN), jnp.float32) * (1.5 * FFN_DIM ** -0.5)).astype(jnp.bfloat16)
    return {'tokens': tokens, 'grad_out': grad_out, 'w_up': w_up, 'w_down': w_down}


def rms_norm(x_f32):
    return x_f32 * lax.rsqrt(jnp.mean(x_f32 * x_f32, axis=-1, keepdims=True) + NORM_EPS)


def gelu_tanh(values):
    return jax.nn.gelu(values, approximate=True)


def layer_forward(layer_in, up_w, down_w):
    x_f32 = layer_in.astype(jnp.float32)
    normed = rms_norm(x_f32).astype(jnp.bfloat16)
    pre_act = jnp.dot(normed, up_w, preferred_element_type=jnp.float32).astype(jnp.bfloat16)
    hidden = gelu_tanh(pre_act.astype(jnp.float32)).astype(jnp.bfloat16)
    return (x_f32 + jnp.dot(hidden, down_w, preferred_element_type=jnp.float32)).astype(jnp.bfloat16)


def layer_backward(layer_in, cotangent, up_w, down_w):
    x_f32 = layer_in.astype(jnp.float32)
    normed = rms_norm(x_f32).astype(jnp.bfloat16)
    pre_act = jnp.dot(normed, up_w, preferred_element_type=jnp.float32).astype(jnp.bfloat16)
    hidden = gelu_tanh(pre_act.astype(jnp.float32)).astype(jnp.bfloat16)
    grad_down = jnp.dot(hidden.T, cotangent, preferred_element_type=jnp.float32)
    d_hidden = jnp.dot(cotangent, down_w.T, preferred_element_type=jnp.float32).astype(jnp.bfloat16)
    _, gelu_back = jax.vjp(gelu_tanh, pre_act.astype(jnp.float32))
    d_pre = gelu_back(d_hidden.astype(jnp.float32))[0].astype(jnp.bfloat16)
    grad_up = jnp.dot(normed.T, d_pre, preferred_element_type=jnp.float32)
    d_normed = jnp.dot(d_pre, up_w.T, preferred_element_type=jnp.float32)
    _, norm_back = jax.vjp(rms_norm, x_f32)
    d_input = (cotangent.astype(jnp.float32) + norm_back(d_normed)[0]).astype(jnp.bfloat16)
    return d_input, grad_up, grad_down


def reference(tokens, grad_out, w_up, w_down):
    n_blocks = TOTAL_TOKENS // BLOCK_ROWS
    tok_blocks = tokens.reshape(n_blocks, BLOCK_ROWS, HIDDEN)
    grad_blocks = grad_out.reshape(n_blocks, BLOCK_ROWS, HIDDEN)

    def block_step(grad_accum, block_pair):
        accum_up, accum_down = grad_accum
        x_block, g_block = block_pair

        def fwd_step(hidden_state, weights):
            up_w, down_w = weights
            return layer_forward(hidden_state, up_w, down_w), hidden_state

        x_final, layer_inputs = lax.scan(fwd_step, x_block, (w_up, w_down))

        def bwd_step(cotangent, layer_items):
            layer_in, up_w, down_w = layer_items
            d_input, grad_up, grad_down = layer_backward(layer_in, cotangent, up_w, down_w)
            return d_input, (grad_up, grad_down)

        d_tokens, layer_grads = lax.scan(bwd_step, g_block, (layer_inputs, w_up, w_down), reverse=True)
        return (accum_up + layer_grads[0], accum_down + layer_grads[1]), (x_final, d_tokens)

    start_accum = (jnp.zeros((NUM_LAYERS, HIDDEN, FFN_DIM), jnp.float32), jnp.zeros((NUM_LAYERS, FFN_DIM, HIDDEN), jnp.float32))
    total_grads, block_outs = lax.scan(block_step, start_accum, (tok_blocks, grad_blocks))
    x_out = block_outs[0].reshape(TOTAL_TOKENS, HIDDEN)
    dx_in = block_outs[1].reshape(TOTAL_TOKENS, HIDDEN)
    return (x_out, dx_in, total_grads[0], total_grads[1])
```

```python
import jax
import jax.numpy as jnp
from jax import lax
from jax.sharding import Mesh, PartitionSpec as P

NORM_EPS = 1e-6
ALL_AXES = ('y', 'x', 'core')
CHIPS = ('y', 'x')
SWAP = [(0, 1), (1, 0)]
CONTRACT_ROWS = (((0,), (0,)), ((), ()))
CONTRACT_COLS = (((1,), (1,)), ((), ()))
CONTRACT_MID = (((1,), (0,)), ((), ()))


def rms_norm(x_f32):
    return x_f32 * lax.rsqrt(jnp.mean(x_f32 * x_f32, axis=-1, keepdims=True) + NORM_EPS)


def gelu_tanh(values):
    return jax.nn.gelu(values, approximate=True)


def dot(a, b, dims=CONTRACT_MID):
    return lax.dot_general(a, b, dims, preferred_element_type=jnp.float32)


def partner(value):
    return lax.ppermute(value, 'core', SWAP)


def with_partner(value):
    return jnp.concatenate([value, partner(value)], axis=0)


def after(value, *others):
    return lax.optimization_barrier((value, *others))[0]


def solution(mesh):
    n_y = mesh.shape['local']
    n_x = mesh.shape['data'] // 2
    n_chips = n_y * n_x
    mesh3 = Mesh(mesh.devices.reshape(n_y, n_x, 2), ALL_AXES)
    tok_spec = P(ALL_AXES, None)
    w_spec = P(None, ALL_AXES, None)

    def device_fn(tokens, grad_out, w_up, w_down):
        even = lax.axis_index('core') == 0
        rows, _ = w_up.shape[1:]
        blk = w_down.shape[1]
        n_tok = tokens.shape[0]

        def pair_columns(w):
            even_cols = jnp.concatenate([w[:, (2 * k) * blk:(2 * k + 1) * blk] for k in range(n_chips)], axis=1)
            odd_cols = jnp.concatenate([w[:, (2 * k + 1) * blk:(2 * k + 2) * blk] for k in range(n_chips)], axis=1)
            mine = jnp.where(even, even_cols, odd_cols)
            other = partner(jnp.where(even, odd_cols, even_cols))
            return jnp.stack([jnp.where(even, mine, other), jnp.where(even, other, mine)])

        def chips_gather(value):
            return lax.all_gather(value, CHIPS, axis=0, tiled=False)

        def chips_scatter(value):
            return lax.psum_scatter(value, CHIPS, scatter_dimension=0, tiled=True)

        def half_sum(lhs, rhs, dims):
            theirs = partner(dot(lhs[n_tok:], rhs, dims))
            return dot(lhs[:n_tok], rhs, dims) + theirs

        def chips_gather_by_permute(value):
            top = value.shape[0] // 2
            from_x = lax.ppermute(value, 'x', SWAP)
            from_y = lax.ppermute(value, 'y', SWAP)
            diag = jnp.concatenate([lax.ppermute(from_x[:top], 'y', SWAP), lax.ppermute(from_y[top:], 'x', SWAP)])
            x_odd = lax.axis_index('x') == 1
            y_odd = lax.axis_index('y') == 1
            pair = [jnp.where(x_odd, p, q) for p, q in ((from_x, value), (value, from_x))]
            far = [jnp.where(x_odd, p, q) for p, q in ((diag, from_y), (from_y, diag))]
            return jnp.stack([jnp.where(y_odd, f, p) for p, f in zip(pair, far)] + [jnp.where(y_odd, p, f) for p, f in zip(pair, far)])

        def row_block(result):
            keep = jnp.where(even, result[:rows], result[rows:])
            recv = partner(jnp.where(even, result[rows:], result[:rows]))
            first = jnp.where(even, keep, recv)
            second = jnp.where(even, recv, keep)
            parts = []
            for k in range(n_chips):
                parts += [first[:, k * blk:(k + 1) * blk], second[:, k * blk:(k + 1) * blk]]
            return jnp.concatenate(parts, axis=1)

        def gelu_bwd(pre_act, d_hidden):
            _, back = jax.vjp(gelu_tanh, pre_act.astype(jnp.float32))
            return back(d_hidden.astype(jnp.float32))[0].astype(jnp.bfloat16)

        def norm_bwd(x, cotangent, d_normed):
            _, back = jax.vjp(rms_norm, x.astype(jnp.float32))
            return (cotangent.astype(jnp.float32) + back(d_normed)[0]).astype(jnp.bfloat16)

        def normed(x):
            return rms_norm(x.astype(jnp.float32)).astype(jnp.bfloat16)

        up0 = pair_columns(w_up[0])
        hid = n_chips * 2 * rows
        gat0 = chips_gather(up0)
        full_up0 = gat0.reshape(hid, -1)
        norm0 = with_partner(normed(tokens))
        up1 = pair_columns(after(w_up[1], up0, norm0))
        down0 = chips_gather(w_down[0]).reshape(n_chips * blk, -1)
        full_up1 = chips_gather(up1).reshape(hid, -1)
        down1 = chips_gather(w_down[1]).reshape(n_chips * blk, -1)

        pre0 = dot(norm0, full_up0).astype(jnp.bfloat16)
        kept0 = after(gat0[:, 0], pre0)
        hid0 = gelu_tanh(pre0.astype(jnp.float32)).astype(jnp.bfloat16)
        x1 = (tokens.astype(jnp.float32) + half_sum(hid0, down0, CONTRACT_MID)).astype(jnp.bfloat16)

        norm1 = with_partner(normed(x1))
        pre1 = dot(norm1, full_up1).astype(jnp.bfloat16)
        hid1 = gelu_tanh(pre1.astype(jnp.float32)).astype(jnp.bfloat16)
        g_pair = with_partner(grad_out)
        g_down1 = chips_scatter(dot(hid1, g_pair, CONTRACT_ROWS))
        again0 = chips_gather_by_permute(after(up0[1], pre1))

        d_hid1 = dot(g_pair, down1, CONTRACT_COLS).astype(jnp.bfloat16)
        d_pre1 = gelu_bwd(pre1, d_hid1)
        g_up1 = chips_scatter(dot(norm1, d_pre1, CONTRACT_ROWS))
        dx1 = norm_bwd(x1, grad_out, half_sum(d_pre1, full_up1, CONTRACT_COLS))

        dx1_pair = with_partner(dx1)
        d_hid0 = dot(dx1_pair, down0, CONTRACT_COLS).astype(jnp.bfloat16)
        d_pre0 = gelu_bwd(pre0, d_hid0)
        g_up0 = chips_scatter(dot(norm0, d_pre0, CONTRACT_ROWS))
        g_down0 = chips_scatter(dot(hid0, dx1_pair, CONTRACT_ROWS))
        x_out = (x1.astype(jnp.float32) + half_sum(hid1, down1, CONTRACT_MID)).astype(jnp.bfloat16)
        full_up0_again = jnp.stack([kept0, again0], axis=1).reshape(hid, -1)
        dx0 = norm_bwd(tokens, dx1, half_sum(d_pre0, full_up0_again, CONTRACT_COLS))

        blocks_up = [row_block(g_up0), row_block(g_up1)]
        grad_up = jnp.stack(blocks_up)
        grad_down = lax.optimization_barrier(jnp.stack([g_down1, g_down1]))
        grad_down = lax.dynamic_update_slice(grad_down, g_down0[None], (0, 0, 0))
        return x_out, dx0, grad_up, grad_down

    return jax.shard_map(device_fn, mesh=mesh3, in_specs=(tok_spec, tok_spec, w_spec, w_spec), out_specs=(tok_spec, tok_spec, w_spec, w_spec), check_vma=False)
```

```python
import jax
import jax.numpy as jnp
from jax import lax
from jax.experimental import pallas as pl
from jax.sharding import Mesh, PartitionSpec as P

NORM_EPS = 1e-6
ROW_TILE = 32
PIECES = 2
ALL_AXES = ('y', 'x', 'core')
CHIPS = ('y', 'x')
SWAP = [(0, 1), (1, 0)]
CONTRACT_ROWS = (((0,), (0,)), ((), ()))
CONTRACT_COLS = (((1,), (1,)), ((), ()))
CONTRACT_MID = (((1,), (0,)), ((), ()))


def rms_norm(x_f32):
    return x_f32 * lax.rsqrt(jnp.mean(x_f32 * x_f32, axis=-1, keepdims=True) + NORM_EPS)


def gelu_tanh(values):
    return jax.nn.gelu(values, approximate=True)


def dot(a, b, dims=CONTRACT_MID):
    return lax.dot_general(a, b, dims, preferred_element_type=jnp.float32)


def partner(value):
    return lax.ppermute(value, 'core', SWAP)


def with_partner(value):
    return jnp.concatenate([value, partner(value)], axis=0)


def after(value, *others):
    return lax.optimization_barrier((value, *others))[0]


def solution(mesh):
    n_y = mesh.shape['local']
    n_x = mesh.shape['data'] // 2
    n_chips = n_y * n_x
    mesh3 = Mesh(mesh.devices.reshape(n_y, n_x, 2), ALL_AXES)
    tok_spec = P(ALL_AXES, None)
    w_spec = P(None, ALL_AXES, None)

    def device_fn(tokens, grad_out, w_up, w_down):
        even = lax.axis_index('core') == 0
        rows, ffn = w_up.shape[1:]
        blk = w_down.shape[1]
        n_tok = tokens.shape[0]

        def pick(layer):
            def kernel(w_ref, mine_ref, other_ref):
                is_even = lax.axis_index('core') == 0

                def copy(first, mine, other):
                    for k in range(n_chips):
                        dst = slice(k * blk, (k + 1) * blk)
                        mine[:, dst] = w_ref[:, (2 * k + first) * blk:(2 * k + first + 1) * blk]
                        other[:, dst] = w_ref[:, (2 * k + 1 - first) * blk:(2 * k + 2 - first) * blk]

                @pl.when(is_even)
                def _():
                    copy(0, mine_ref, other_ref)

                @pl.when(jnp.logical_not(is_even))
                def _():
                    copy(1, mine_ref, other_ref)

            half = jax.ShapeDtypeStruct((rows, ffn // 2), w_up.dtype)
            spec = pl.BlockSpec((ROW_TILE, ffn // 2), lambda i: (i, 0))
            return pl.pallas_call(
                kernel, grid=(rows // ROW_TILE,), out_shape=(half, half),
                in_specs=[pl.BlockSpec((None, ROW_TILE, ffn), lambda i: (layer, i, 0))], out_specs=(spec, spec), name='pick')

        def join(mine, other):
            def kernel(mine_ref, other_ref, out_ref):
                is_even = lax.axis_index('core') == 0

                @pl.when(is_even)
                def _():
                    out_ref[0] = mine_ref[...]
                    out_ref[1] = other_ref[...]

                @pl.when(jnp.logical_not(is_even))
                def _():
                    out_ref[0] = other_ref[...]
                    out_ref[1] = mine_ref[...]

            spec = pl.BlockSpec((ROW_TILE, ffn // 2), lambda i: (i, 0))
            return pl.pallas_call(
                kernel, grid=(rows // ROW_TILE,), out_shape=jax.ShapeDtypeStruct((2, rows, ffn // 2), w_up.dtype),
                in_specs=[spec, spec], out_specs=pl.BlockSpec((2, ROW_TILE, ffn // 2), lambda i: (0, i, 0)), name='join')(mine, other)

        def pair_columns(w, layer):
            mine, other = pick(layer)(w)
            return join(mine, partner(other))

        whole_spec = pl.BlockSpec((1, 2, ROW_TILE, ffn // 2), lambda c, i: (c, 0, i, 0))
        part_spec = pl.BlockSpec((1, ROW_TILE, ffn // 2), lambda c, i: (c, i, 0))
        part_shape = jax.ShapeDtypeStruct((n_chips, rows, ffn // 2), w_up.dtype)
        part_grid = (n_chips, rows // ROW_TILE)

        def split(whole):
            def kernel(whole_ref, keep_ref, give_ref):
                is_even = lax.axis_index('core') == 0

                @pl.when(is_even)
                def _():
                    keep_ref[...] = whole_ref[:, 0]
                    give_ref[...] = whole_ref[:, 1]

                @pl.when(jnp.logical_not(is_even))
                def _():
                    keep_ref[...] = whole_ref[:, 1]
                    give_ref[...] = whole_ref[:, 0]

            return pl.pallas_call(kernel, grid=part_grid, out_shape=(part_shape, part_shape), in_specs=[whole_spec], out_specs=(part_spec, part_spec), name='split')(whole)

        def merge(kept, taken):
            def kernel(keep_ref, take_ref, whole_ref):
                is_even = lax.axis_index('core') == 0

                @pl.when(is_even)
                def _():
                    whole_ref[:, 0] = keep_ref[...]
                    whole_ref[:, 1] = take_ref[...]

                @pl.when(jnp.logical_not(is_even))
                def _():
                    whole_ref[:, 0] = take_ref[...]
                    whole_ref[:, 1] = keep_ref[...]

            shape = jax.ShapeDtypeStruct((n_chips, 2, rows, ffn // 2), w_up.dtype)
            return pl.pallas_call(kernel, grid=part_grid, out_shape=shape, in_specs=[part_spec, part_spec], out_specs=whole_spec, name='merge')(kept, taken)

        def chips_gather(value):
            return lax.all_gather(value, CHIPS, axis=0, tiled=False)

        def chips_scatter(value):
            return lax.psum_scatter(value, CHIPS, scatter_dimension=0, tiled=True)

        def half_sum(lhs, rhs, dims, pieces=1):
            step = n_tok // pieces
            theirs = [partner(dot(lhs[n_tok + i * step:n_tok + (i + 1) * step], rhs, dims)) for i in range(pieces)]
            return [dot(lhs[i * step:(i + 1) * step], rhs, dims) + theirs[i] for i in range(pieces)]

        def row_block(result):
            keep = jnp.where(even, result[:rows], result[rows:])
            recv = partner(jnp.where(even, result[rows:], result[:rows]))
            first = jnp.where(even, keep, recv)
            second = jnp.where(even, recv, keep)
            parts = []
            for k in range(n_chips):
                parts += [first[:, k * blk:(k + 1) * blk], second[:, k * blk:(k + 1) * blk]]
            return jnp.concatenate(parts, axis=1)

        def gelu_bwd(pre_act, d_hidden):
            _, back = jax.vjp(gelu_tanh, pre_act.astype(jnp.float32))
            return back(d_hidden.astype(jnp.float32))[0].astype(jnp.bfloat16)

        def norm_bwd(x, cotangent, d_normed):
            _, back = jax.vjp(rms_norm, x.astype(jnp.float32))
            return (cotangent.astype(jnp.float32) + back(d_normed)[0]).astype(jnp.bfloat16)

        def normed(x):
            return rms_norm(x.astype(jnp.float32)).astype(jnp.bfloat16)

        up0 = pair_columns(w_up, 0)
        hid = n_chips * 2 * rows
        gat0 = chips_gather(up0)
        full_up0 = gat0.reshape(hid, -1)
        norm0 = with_partner(normed(tokens))
        up1 = pair_columns(after(w_up, up0, norm0), 1)
        down0 = chips_gather(w_down[0]).reshape(n_chips * blk, -1)
        full_up1 = chips_gather(up1).reshape(hid, -1)
        down1 = chips_gather(w_down[1]).reshape(n_chips * blk, -1)

        pre0 = dot(norm0, full_up0).astype(jnp.bfloat16)
        kept0, given0 = split(after(gat0, pre0))
        kept0, taken0 = lax.optimization_barrier((kept0, partner(given0)))
        hid0 = gelu_tanh(pre0.astype(jnp.float32)).astype(jnp.bfloat16)
        sums0 = half_sum(hid0, down0, CONTRACT_MID, PIECES)
        step = n_tok // PIECES
        x1 = [(tokens[i * step:(i + 1) * step].astype(jnp.float32) + sums0[i]).astype(jnp.bfloat16) for i in range(PIECES)]
        norms1 = [normed(v) for v in x1]
        norm1 = jnp.concatenate(norms1 + [partner(v) for v in norms1])
        x1 = jnp.concatenate(x1)
        pre1 = dot(norm1, full_up1).astype(jnp.bfloat16)
        hid1 = gelu_tanh(pre1.astype(jnp.float32)).astype(jnp.bfloat16)
        g_pair = with_partner(grad_out)
        g_down1 = chips_scatter(dot(hid1, g_pair, CONTRACT_ROWS))
        d_hid1 = dot(g_pair, down1, CONTRACT_COLS).astype(jnp.bfloat16)
        d_pre1 = gelu_bwd(pre1, d_hid1)
        g_up1 = chips_scatter(dot(norm1, d_pre1, CONTRACT_ROWS))
        dx1 = norm_bwd(x1, grad_out, half_sum(d_pre1, full_up1, CONTRACT_COLS)[0])

        dx1_pair = with_partner(dx1)
        d_hid0 = dot(dx1_pair, down0, CONTRACT_COLS).astype(jnp.bfloat16)
        d_pre0 = gelu_bwd(pre0, d_hid0)
        g_up0 = chips_scatter(dot(norm0, d_pre0, CONTRACT_ROWS))
        g_down0 = chips_scatter(dot(hid0, dx1_pair, CONTRACT_ROWS))
        x_out = (x1.astype(jnp.float32) + half_sum(hid1, down1, CONTRACT_MID)[0]).astype(jnp.bfloat16)
        again0 = partner(taken0)
        full_up0_again = merge(kept0, again0).reshape(hid, -1)
        dx0 = norm_bwd(tokens, dx1, half_sum(d_pre0, full_up0_again, CONTRACT_COLS)[0])

        blocks_up = [row_block(g_up0), row_block(g_up1)]
        grad_up = jnp.stack(blocks_up)
        grad_down = lax.optimization_barrier(jnp.stack([g_down1, g_down1]))
        grad_down = lax.dynamic_update_slice(grad_down, g_down0[None], (0, 0, 0))
        return x_out, dx0, grad_up, grad_down

    return jax.shard_map(device_fn, mesh=mesh3, in_specs=(tok_spec, tok_spec, w_spec, w_spec), out_specs=(tok_spec, tok_spec, w_spec, w_spec), check_vma=False)
```

```python
import jax
import jax.numpy as jnp
from jax import lax
from jax.experimental import pallas as pl
from jax.sharding import Mesh, PartitionSpec as P

NORM_EPS = 1e-6
ROW_TILE = 32
PIECES = 2
ALL_AXES = ('y', 'x', 'core')
CHIPS = ('y', 'x')
SWAP = [(0, 1), (1, 0)]
CONTRACT_ROWS = (((0,), (0,)), ((), ()))
CONTRACT_COLS = (((1,), (1,)), ((), ()))
CONTRACT_MID = (((1,), (0,)), ((), ()))


def rms_norm(x_f32):
    return x_f32 * lax.rsqrt(jnp.mean(x_f32 * x_f32, axis=-1, keepdims=True) + NORM_EPS)


def gelu_tanh(values):
    return jax.nn.gelu(values, approximate=True)


def dot(a, b, dims=CONTRACT_MID):
    return lax.dot_general(a, b, dims, preferred_element_type=jnp.float32)


def partner(value):
    return lax.ppermute(value, 'core', SWAP)


def with_partner(value):
    return jnp.concatenate([value, partner(value)], axis=0)


def solution(mesh):
    n_y = mesh.shape['local']
    n_x = mesh.shape['data'] // 2
    n_chips = n_y * n_x
    mesh3 = Mesh(mesh.devices.reshape(n_y, n_x, 2), ALL_AXES)
    tok_spec = P(ALL_AXES, None)
    w_spec = P(None, ALL_AXES, None)

    def device_fn(tokens, grad_out, w_up, w_down):
        even = lax.axis_index('core') == 0
        rows, ffn = w_up.shape[1:]
        blk = w_down.shape[1]
        n_tok = tokens.shape[0]

        def pick(whole, first_index, count):
            def kernel(w_ref, mine_ref, other_ref):
                is_even = lax.axis_index('core') == 0

                def copy(first):
                    for k in range(n_chips):
                        dst = slice(k * blk, (k + 1) * blk)
                        mine_ref[:, dst] = w_ref[:, (2 * k + first) * blk:(2 * k + first + 1) * blk]
                        other_ref[:, dst] = w_ref[:, (2 * k + 1 - first) * blk:(2 * k + 2 - first) * blk]

                @pl.when(is_even)
                def _():
                    copy(0)

                @pl.when(jnp.logical_not(is_even))
                def _():
                    copy(1)

            half = jax.ShapeDtypeStruct((count, rows, ffn // 2), w_up.dtype)
            spec = pl.BlockSpec((None, ROW_TILE, ffn // 2), lambda c, i: (c, i, 0))
            return pl.pallas_call(
                kernel, grid=(count, rows // ROW_TILE), out_shape=(half, half),
                in_specs=[pl.BlockSpec((None, ROW_TILE, ffn), lambda c, i: (c + first_index, i, 0))], out_specs=(spec, spec), name='pick')(whole)

        def join(mine, other):
            def kernel(mine_ref, other_ref, out_ref):
                is_even = lax.axis_index('core') == 0

                @pl.when(is_even)
                def _():
                    out_ref[0] = mine_ref[...]
                    out_ref[1] = other_ref[...]

                @pl.when(jnp.logical_not(is_even))
                def _():
                    out_ref[0] = other_ref[...]
                    out_ref[1] = mine_ref[...]

            spec = pl.BlockSpec((ROW_TILE, ffn // 2), lambda i: (i, 0))
            return pl.pallas_call(
                kernel, grid=(rows // ROW_TILE,), out_shape=jax.ShapeDtypeStruct((2, rows, ffn // 2), w_up.dtype),
                in_specs=[spec, spec], out_specs=pl.BlockSpec((2, ROW_TILE, ffn // 2), lambda i: (0, i, 0)), name='join')(mine, other)

        def pair_columns(w, layer):
            mine, other = pick(w, layer, 1)
            return join(mine[0], partner(other[0]))

        whole_spec = pl.BlockSpec((1, 2, ROW_TILE, ffn // 2), lambda c, i: (c, 0, i, 0))
        part_spec = pl.BlockSpec((1, ROW_TILE, ffn // 2), lambda c, i: (c, i, 0))
        part_grid = (n_chips, rows // ROW_TILE)

        def merge(kept, taken):
            def kernel(keep_ref, take_ref, whole_ref):
                is_even = lax.axis_index('core') == 0

                @pl.when(is_even)
                def _():
                    whole_ref[:, 0] = keep_ref[...]
                    whole_ref[:, 1] = take_ref[...]

                @pl.when(jnp.logical_not(is_even))
                def _():
                    whole_ref[:, 0] = take_ref[...]
                    whole_ref[:, 1] = keep_ref[...]

            shape = jax.ShapeDtypeStruct((n_chips, 2, rows, ffn // 2), w_up.dtype)
            return pl.pallas_call(kernel, grid=part_grid, out_shape=shape, in_specs=[part_spec, part_spec], out_specs=whole_spec, name='merge')(kept, taken)

        def chips_gather(value):
            return lax.all_gather(value, CHIPS, axis=0, tiled=False)

        def chips_scatter(value):
            return lax.psum_scatter(value, CHIPS, scatter_dimension=0, tiled=True)

        def half_sum(lhs, rhs, dims, pieces=1):
            step = n_tok // pieces
            theirs = [partner(dot(lhs[n_tok + i * step:n_tok + (i + 1) * step], rhs, dims)) for i in range(pieces)]
            return [dot(lhs[i * step:(i + 1) * step], rhs, dims) + theirs[i] for i in range(pieces)]

        def row_block(result):
            keep = jnp.where(even, result[:rows], result[rows:])
            recv = partner(jnp.where(even, result[rows:], result[:rows]))
            first = jnp.where(even, keep, recv)
            second = jnp.where(even, recv, keep)
            parts = []
            for k in range(n_chips):
                parts += [first[:, k * blk:(k + 1) * blk], second[:, k * blk:(k + 1) * blk]]
            return jnp.concatenate(parts, axis=1)

        def gelu_bwd(pre_act, d_hidden):
            _, back = jax.vjp(gelu_tanh, pre_act.astype(jnp.float32))
            return back(d_hidden.astype(jnp.float32))[0].astype(jnp.bfloat16)

        def norm_bwd(x, cotangent, d_normed):
            _, back = jax.vjp(rms_norm, x.astype(jnp.float32))
            return (cotangent.astype(jnp.float32) + back(d_normed)[0]).astype(jnp.bfloat16)

        def normed(x):
            return rms_norm(x.astype(jnp.float32)).astype(jnp.bfloat16)

        hid = n_chips * 2 * rows
        mine0, other0 = pick(chips_gather(w_up[0]), 0, n_chips)
        full_up0 = merge(mine0, partner(other0)).reshape(hid, -1)
        norm0 = with_partner(normed(tokens))
        up1 = pair_columns(w_up, 1)
        down0 = chips_gather(w_down[0]).reshape(n_chips * blk, -1)
        full_up1 = chips_gather(up1).reshape(hid, -1)
        down1 = chips_gather(w_down[1]).reshape(n_chips * blk, -1)

        pre0 = dot(norm0, full_up0).astype(jnp.bfloat16)
        mine0, other0 = lax.optimization_barrier((mine0, other0, pre0))[:2]
        hid0 = gelu_tanh(pre0.astype(jnp.float32)).astype(jnp.bfloat16)
        sums0 = half_sum(hid0, down0, CONTRACT_MID, PIECES)
        step = n_tok // PIECES
        x1 = [(tokens[i * step:(i + 1) * step].astype(jnp.float32) + sums0[i]).astype(jnp.bfloat16) for i in range(PIECES)]
        norms1 = [normed(v) for v in x1]
        norm1 = jnp.concatenate(norms1 + [partner(v) for v in norms1])
        x1 = jnp.concatenate(x1)
        pre1 = dot(norm1, full_up1).astype(jnp.bfloat16)
        hid1 = gelu_tanh(pre1.astype(jnp.float32)).astype(jnp.bfloat16)
        g_pair = with_partner(grad_out)
        g_down1 = chips_scatter(dot(hid1, g_pair, CONTRACT_ROWS))
        d_hid1 = dot(g_pair, down1, CONTRACT_COLS).astype(jnp.bfloat16)
        d_pre1 = gelu_bwd(pre1, d_hid1)
        g_up1 = chips_scatter(dot(norm1, d_pre1, CONTRACT_ROWS))
        dx1 = norm_bwd(x1, grad_out, half_sum(d_pre1, full_up1, CONTRACT_COLS)[0])

        dx1_pair = with_partner(dx1)
        d_hid0 = dot(dx1_pair, down0, CONTRACT_COLS).astype(jnp.bfloat16)
        d_pre0 = gelu_bwd(pre0, d_hid0)
        g_up0 = chips_scatter(dot(norm0, d_pre0, CONTRACT_ROWS))
        g_down0 = chips_scatter(dot(hid0, dx1_pair, CONTRACT_ROWS))
        x_out = (x1.astype(jnp.float32) + half_sum(hid1, down1, CONTRACT_MID)[0]).astype(jnp.bfloat16)
        again0 = partner(other0)
        full_up0_again = merge(mine0, again0).reshape(hid, -1)
        dx0 = norm_bwd(tokens, dx1, half_sum(d_pre0, full_up0_again, CONTRACT_COLS)[0])

        blocks_up = [row_block(g_up0), row_block(g_up1)]
        grad_up = jnp.stack(blocks_up)
        grad_down = lax.optimization_barrier(jnp.stack([g_down1, g_down1]))
        grad_down = lax.dynamic_update_slice(grad_down, g_down0[None], (0, 0, 0))
        return x_out, dx0, grad_up, grad_down

    return jax.shard_map(device_fn, mesh=mesh3, in_specs=(tok_spec, tok_spec, w_spec, w_spec), out_specs=(tok_spec, tok_spec, w_spec, w_spec), check_vma=False)
```
